32 devices in a mesh: grp: 2 (over y), res: 8 (over z, x), seq: 2 (over core).
Axes of the slice: x: 2, y: 2, z: 4, core: 2. Of those that a mesh axis runs over, the one named last changes fastest.
Arguments:
- aligned_activity: bfloat16 [512, 512, 256], P(('grp', 'seq'), 'res'), parts along dimension 0, may hold values from -6 to 6
- pair_state: bfloat16 [1024, 512, 128], P(('grp', 'res'), 'seq'), parts along dimension 0, may hold values from -6 to 6
- focus_scaling_vector: float32 [256], replicated, may hold values from 0.5 to 2
- combined_probe_matrix: bfloat16 [256, 1024], replicated, may hold values from -0.375 to 0.375
- sigmoid_offset_vector: float32 [256], replicated, may hold values from -4 to 4
- focus_final_matrix: bfloat16 [256, 256], replicated, may hold values from -0.375 to 0.375
- pair_norm_gain: float32 [128], replicated, may hold values from 0.5 to 2
- pair_bias_matrix: float32 [128, 8], replicated, may hold values from -36 to 36
- feedforward_scaling_vector: float32 [256], replicated, may hold values from 0.5 to 2
- feedforward_widen_matrix: bfloat16 [256, 1024], replicated, may hold values from -0.375 to 0.375
- feedforward_shrink_matrix: bfloat16 [1024, 256], replicated, may hold values from -0.1875 to 0.1875
- tensor_scaling_vector: float32 [256], replicated, may hold values from 0.5 to 2
- twin_operand_matrix: bfloat16 [256, 64], replicated, may hold values from -0.375 to 0.375
- tensor_final_matrix: bfloat16 [1024, 128], replicated, may hold values from -3 to 3
Outputs:
- alignment_output: bfloat16 [512, 512, 256], P(('grp', 'seq'), 'res'), parts along dimension 0
- pair_output: bfloat16 [1024, 512, 128], P(('grp', 'res'), 'seq'), parts along dimension 0
The draws below stay inside these ranges and needn't reach their ends.
There are 2 independent parts, one for each index of `grp`. The reference program is written for one: setup_inputs(seed, part) draws one part's arguments, and reference() takes and returns one part's arrays. A program takes and returns all parts, laid end to end along the dimension named above; an argument that names none is the same for every part. Nothing has to cross between parts.
All inputs are finite; a program needn't handle non-finite values.
Results may differ from the reference program's by a relative error of at most 0.0095.
The reference program's roundings to bfloat16 on the way count: a program that leaves them out, or rounds other values in their place, can miss the bound.
Values may be sent and summed in bfloat16 or wider, within the bound.
A program may use at most 256 MiB of HBM per device.

```python
import math
import jax
import jax.numpy as jnp
from jax import lax

ALIGNED_DEPTH = 256
COUPLING_DEPTH = 128
FOCUS_GROUPS = 8
PRODUCT_DEPTH = 32
ALIGNED_CHAINS = 256
AMINO_SITES = 512
HIDDEN_UNITS = 1024
N_RES = 8


def draw_pair_bias_matrix(key, part):
    raw = jnp.clip(jax.random.normal(key, (COUPLING_DEPTH, FOCUS_GROUPS), jnp.float32), -4.0, 4.0)
    return raw * 0.09


def level_of(rng, shape, split, low, largest):
    gain = 1.0
    for position, parts in split:
        steps = jax.random.uniform(jax.random.fold_in(jax.random.fold_in(rng, 6), position), (parts,), jnp.float32, low / len(split), largest / len(split))
        gain = gain * jnp.repeat(jnp.exp(steps), shape[position] // parts).reshape((-1,) + (1,) * (len(shape) - 1 - position))
    return gain


def normal_values(own_key, extent, width, reach, split=(), held_as=jnp.bfloat16):
    entries = jax.random.normal(own_key, extent, jnp.float32) * width
    if len(split) > 0:
        entries = level_of(own_key, extent, split, -0.22, 0.18) * entries
    return jnp.clip(entries, min=-reach, max=reach).astype(held_as)


def setup_inputs(seed: int = 0, part: int = 0) -> dict:
    splits = jax.random.split(jax.random.key(seed), 15)
    own_keys = jax.random.split(jax.random.fold_in(splits[14], part), 15)
    aligned_activity = normal_values(own_keys[0], (ALIGNED_CHAINS, AMINO_SITES, ALIGNED_DEPTH), 1.0, 6.0, ((0, 2), (1, 8)))
    pair_state = normal_values(own_keys[1], (AMINO_SITES, AMINO_SITES, COUPLING_DEPTH), 1.0, 6.0, ((0, 8), (1, 2)))
    focus_scaling_vector = jnp.clip(jnp.exp(jax.random.uniform(splits[2], (ALIGNED_DEPTH,), jnp.float32, math.log(0.5), math.log(2.0))), 0.5, 2.0)
    combined_probe_matrix = normal_values(splits[3], (ALIGNED_DEPTH, 4 * ALIGNED_DEPTH), ALIGNED_DEPTH ** -0.5, 0.375)
    sigmoid_offset_vector = normal_values(splits[4], (ALIGNED_DEPTH,), 1.0, 4.0, (), jnp.float32)
    focus_final_matrix = normal_values(splits[5], (ALIGNED_DEPTH, ALIGNED_DEPTH), ALIGNED_DEPTH ** -0.5, 0.375)
    pair_norm_gain = jnp.clip(jnp.exp(jax.random.uniform(splits[6], (COUPLING_DEPTH,), jnp.float32, math.log(0.5), math.log(2.0))), 0.5, 2.0)
    pair_bias_matrix = draw_pair_bias_matrix(jax.random.fold_in(splits[14], 71), part)
    feedforward_scaling_vector = jnp.clip(jnp.exp(jax.random.uniform(splits[8], (ALIGNED_DEPTH,), jnp.float32, math.log(0.5), math.log(2.0))), 0.5, 2.0)
    feedforward_widen_matrix = normal_values(splits[9], (ALIGNED_DEPTH, HIDDEN_UNITS), ALIGNED_DEPTH ** -0.5, 0.375)
    feedforward_shrink_matrix = normal_values(splits[10], (HIDDEN_UNITS, ALIGNED_DEPTH), HIDDEN_UNITS ** -0.5, 0.1875)
    tensor_scaling_vector = jnp.clip(jnp.exp(jax.random.uniform(splits[11], (ALIGNED_DEPTH,), jnp.float32, math.log(0.5), math.log(2.0))), 0.5, 2.0)
    twin_operand_matrix = normal_values(splits[12], (ALIGNED_DEPTH, 2 * PRODUCT_DEPTH), ALIGNED_DEPTH ** -0.5, 0.375)
    tensor_final_matrix = normal_values(splits[13], (PRODUCT_DEPTH * PRODUCT_DEPTH, COUPLING_DEPTH), (max(1, PRODUCT_DEPTH * PRODUCT_DEPTH // ALIGNED_CHAINS)) ** -0.5, 3.0)
    return dict(aligned_activity=aligned_activity, pair_state=pair_state, focus_scaling_vector=focus_scaling_vector, combined_probe_matrix=combined_probe_matrix, sigmoid_offset_vector=sigmoid_offset_vector, focus_final_matrix=focus_final_matrix, pair_norm_gain=pair_norm_gain, pair_bias_matrix=pair_bias_matrix, feedforward_scaling_vector=feedforward_scaling_vector, feedforward_widen_matrix=feedforward_widen_matrix, feedforward_shrink_matrix=feedforward_shrink_matrix, tensor_scaling_vector=tensor_scaling_vector, twin_operand_matrix=twin_operand_matrix, tensor_final_matrix=tensor_final_matrix)


def layer_normalize(inputs, scale_gain):
    sample_expectation = lax.optimization_barrier(jnp.mean(inputs, axis=-1, keepdims=True))
    centered = inputs - sample_expectation
    variance = lax.optimization_barrier(jnp.mean(centered * centered, axis=-1, keepdims=True))
    return centered * lax.rsqrt(variance + 1e-05) * scale_gain

def reference(aligned_activity, pair_state, focus_scaling_vector, combined_probe_matrix, sigmoid_offset_vector, focus_final_matrix, pair_norm_gain, pair_bias_matrix, feedforward_scaling_vector, feedforward_widen_matrix, feedforward_shrink_matrix, tensor_scaling_vector, twin_operand_matrix, tensor_final_matrix):
    subspace_depth = ALIGNED_DEPTH // FOCUS_GROUPS
    probe_multiplier = subspace_depth ** (-0.5)
    pair_norm = layer_normalize(pair_state.astype(jnp.float32), pair_norm_gain)
    pair_bias = jnp.einsum('ijc,ch->hij', pair_norm, pair_bias_matrix, precision=lax.Precision.HIGHEST).astype(jnp.bfloat16)
    bias_wide = pair_bias.astype(jnp.float32)

    def row_attention_update(sequence):
        residual_state = sequence.astype(jnp.float32)
        normalized_rows = layer_normalize(residual_state, focus_scaling_vector).astype(jnp.bfloat16)
        mapped_entries = jnp.dot(normalized_rows, combined_probe_matrix, preferred_element_type=jnp.float32)
        probe_entries = (mapped_entries[:, :ALIGNED_DEPTH] * probe_multiplier).astype(jnp.bfloat16).reshape(AMINO_SITES, FOCUS_GROUPS, subspace_depth)
        lookup_entries = mapped_entries[:, ALIGNED_DEPTH:2 * ALIGNED_DEPTH].astype(jnp.bfloat16).reshape(AMINO_SITES, FOCUS_GROUPS, subspace_depth)
        content_entries = mapped_entries[:, 2 * ALIGNED_DEPTH:3 * ALIGNED_DEPTH].astype(jnp.bfloat16).reshape(AMINO_SITES, FOCUS_GROUPS, subspace_depth)
        sigmoid_filter = jax.nn.sigmoid(mapped_entries[:, 3 * ALIGNED_DEPTH:] + sigmoid_offset_vector)
        scores = jnp.einsum('ihd,jhd->hij', probe_entries.astype(jnp.float32), lookup_entries.astype(jnp.float32)) + bias_wide
        top_score = lax.optimization_barrier(jnp.max(scores, axis=-1, keepdims=True))
        exponent = jnp.exp(scores - top_score)
        softmax_shares = (exponent / lax.optimization_barrier(jnp.sum(exponent, axis=-1, keepdims=True))).astype(jnp.bfloat16)
        mixed_entries = jnp.einsum('tnx,xtq->ntq', softmax_shares.astype(jnp.float32), content_entries.astype(jnp.float32)).reshape(AMINO_SITES, ALIGNED_DEPTH)
        gated_rows = (mixed_entries * sigmoid_filter).astype(jnp.bfloat16)
        residual_state = residual_state + jnp.dot(gated_rows, focus_final_matrix, preferred_element_type=jnp.float32)
        normalized_rows = layer_normalize(residual_state, feedforward_scaling_vector).astype(jnp.bfloat16)
        hidden = jnp.maximum(jnp.dot(normalized_rows, feedforward_widen_matrix, preferred_element_type=jnp.float32), 0.0).astype(jnp.bfloat16)
        residual_state = residual_state + jnp.dot(hidden, feedforward_shrink_matrix, preferred_element_type=jnp.float32)
        updated_state = residual_state.astype(jnp.bfloat16)
        normalized_rows = layer_normalize(updated_state.astype(jnp.float32), tensor_scaling_vector).astype(jnp.bfloat16)
        left_right_factors = jnp.dot(normalized_rows, twin_operand_matrix, preferred_element_type=jnp.float32).astype(jnp.bfloat16)
        return (updated_state, left_right_factors)
    alignment_output, left_right_factors = lax.map(row_attention_update, aligned_activity)
    left_fac = left_right_factors[:, :, :PRODUCT_DEPTH].astype(jnp.float32)
    right_fac = left_right_factors[:, :, PRODUCT_DEPTH:].astype(jnp.float32)
    row_block = AMINO_SITES // N_RES
    out_table = tensor_final_matrix.astype(jnp.float32).reshape(PRODUCT_DEPTH, PRODUCT_DEPTH, COUPLING_DEPTH)

    def pair_rows(block_index):
        left_rows = lax.dynamic_slice_in_dim(left_fac, block_index * row_block, row_block, 1)
        tensor_total = jnp.einsum('sic,sje->icje', left_rows, right_fac, precision=lax.Precision.HIGHEST)
        sample_expectation = (tensor_total / ALIGNED_CHAINS).astype(jnp.bfloat16)
        return jnp.einsum('icje,cez->ijz', sample_expectation.astype(jnp.float32), out_table, precision=lax.Precision.HIGHEST)
    update = lax.map(pair_rows, jnp.arange(N_RES, dtype=jnp.int32)).reshape(AMINO_SITES, AMINO_SITES, COUPLING_DEPTH)
    pair_output = (pair_state.astype(jnp.float32) + update).astype(jnp.bfloat16)
    return (alignment_output, pair_output)
```

```python
import functools
import math

import jax
import jax.numpy as jnp
from jax import lax
from jax.experimental import pallas as pl
from jax.experimental.pallas import tpu as pltpu
from jax.sharding import PartitionSpec as P

LOG2E = math.log2(math.e)
VMEM_LIMIT = 60 * 1024 * 1024
CHUNKS = 4


def layer_normalize(inputs, scale_gain):
    sample_expectation = jnp.mean(inputs, axis=-1, keepdims=True)
    centered = inputs - sample_expectation
    variance = jnp.mean(centered * centered, axis=-1, keepdims=True)
    return centered * lax.rsqrt(variance + 1e-05) * scale_gain


def dot_f32(a, b, ca, cb):
    return lax.dot_general(a, b, (((ca,), (cb,)), ((), ())), preferred_element_type=jnp.float32)


def sequence_kernel(
    heads,
    pack,
    x_ref,
    bias_ref,
    gain_ref,
    probe_ref,
    offset_ref,
    final_ref,
    ff_gain_ref,
    widen_ref,
    shrink_ref,
    opm_gain_ref,
    left_w_ref,
    right_w_ref,
    out_ref,
    left_ref,
    right_ref,
    left_acc,
    right_acc,
):
    step = pl.program_id(0)
    steps = right_ref.shape[1]
    blocks, _, rows, width = x_ref.shape
    length = blocks * rows
    depth = width // heads
    x = x_ref[:, 0].astype(jnp.float32).reshape(length, width)
    normed = layer_normalize(x, gain_ref[...]).astype(jnp.bfloat16)
    mapped = dot_f32(probe_ref[...], normed, 1, 1)
    q = (mapped[:width] * (depth ** (-0.5) * LOG2E)).astype(jnp.bfloat16)
    k = mapped[width : 2 * width].astype(jnp.bfloat16)
    v = mapped[2 * width : 3 * width].astype(jnp.bfloat16)
    gate = jax.nn.sigmoid(mapped[3 * width :] + offset_ref[...])
    ones = jnp.ones((16, length), jnp.bfloat16)
    gated = []
    for h in range(heads):
        part = slice(h * depth, (h + 1) * depth)
        scores = dot_f32(k[part], q[part], 0, 0) + bias_ref[h]
        top = jnp.max(scores, axis=0, keepdims=True)
        p = jnp.exp2(scores - top).astype(jnp.bfloat16)
        mixed = dot_f32(jnp.concatenate([v[part], ones], axis=0), p, 1, 0)
        share = mixed[:depth] / mixed[depth : depth + 1]
        gated.append((share * gate[part]).astype(jnp.bfloat16))
    gated = jnp.concatenate(gated, axis=0)
    stream = x + dot_f32(gated, final_ref[...], 0, 0)
    normed = layer_normalize(stream, ff_gain_ref[...]).astype(jnp.bfloat16)
    hidden = jnp.maximum(dot_f32(normed, widen_ref[...], 1, 0), 0.0).astype(jnp.bfloat16)
    stream = stream + dot_f32(hidden, shrink_ref[...], 1, 0)
    updated = stream.astype(jnp.bfloat16)
    out_ref[:, 0] = stream.reshape(blocks, rows, width).astype(jnp.bfloat16)
    normed = layer_normalize(updated.astype(jnp.float32), opm_gain_ref[...]).astype(jnp.bfloat16)
    slot = lax.rem(step, pack)
    left = dot_f32(normed, left_w_ref[slot], 1, 0)

    @pl.when(slot == 0)
    def _():
        left_acc[...] = left

    @pl.when(slot != 0)
    def _():
        left_acc[...] = left_acc[...] + left

    left_ref[:, 0] = left_acc[...].reshape(blocks, rows, left.shape[1]).astype(jnp.bfloat16)
    factor = right_w_ref.shape[0]
    right = dot_f32(right_w_ref[...], normed, 1, 1)
    for e in range(factor):
        right_acc[e, pl.ds(step, 1), :] = right[e : e + 1]

    @pl.when(step == steps - 1)
    def _():
        right_ref[...] = right_acc[...].astype(jnp.bfloat16)


def run_sequences(x, bias, weights, heads, pack):
    blocks, steps, rows, width = x.shape
    length = blocks * rows
    factor = weights[-1].shape[0]
    whole = lambda a: pl.BlockSpec(
        a.shape, lambda s, n=a.ndim: (0,) * n, pipeline_mode=pl.Buffered(1)
    )
    lanes = pack * factor
    hidden = weights[5].shape[1]
    flops = 2 * length * width * (5 * width + 2 * hidden + 128) + 4 * length * length * width
    return pl.pallas_call(
        functools.partial(sequence_kernel, heads, pack),
        grid=(steps,),
        in_specs=[pl.BlockSpec((blocks, 1, rows, width), lambda s: (0, s, 0, 0)), whole(bias)]
        + [whole(a) for a in weights],
        out_specs=[
            pl.BlockSpec((blocks, 1, rows, width), lambda s: (0, s, 0, 0)),
            pl.BlockSpec((blocks, 1, rows, lanes), lambda s: (0, s // pack, 0, 0)),
            pl.BlockSpec((factor, steps, length), lambda s: (0, 0, 0)),
        ],
        out_shape=[
            jax.ShapeDtypeStruct(x.shape, jnp.bfloat16),
            jax.ShapeDtypeStruct((blocks, steps // pack, rows, lanes), jnp.bfloat16),
            jax.ShapeDtypeStruct((factor, steps, length), jnp.bfloat16),
        ],
        scratch_shapes=[
            pltpu.VMEM((length, lanes), jnp.float32),
            pltpu.VMEM((factor, steps, length), jnp.float32),
        ],
        compiler_params=pltpu.CompilerParams(
            dimension_semantics=("arbitrary",), vmem_limit_bytes=VMEM_LIMIT
        ),
        cost_estimate=pl.CostEstimate(
            flops=steps * flops * 3,
            bytes_accessed=bias.size * 4 + 4 * x.size,
            transcendentals=steps * heads * length * length,
        ),
        name="sequences",
    )(x, bias, *weights)


def product_kernel(rows, seq_total, left_ref, right_ref, table_ref, pair_ref, out_ref, stack):
    groups, factor, part, cols = right_ref.shape
    scale = 1.0 / seq_total
    left = left_ref[...]
    for e in range(factor):
        right = right_ref[:, e].reshape(groups * part, cols)
        outer = (dot_f32(left, right, 1, 0) * scale).astype(jnp.bfloat16)
        stack[:, e * factor : (e + 1) * factor, :] = outer.reshape(rows, factor, cols)
    for i in range(rows):
        update = dot_f32(table_ref[...], stack[i], 1, 0)
        out_ref[i] = (pair_ref[i].astype(jnp.float32) + update.T).astype(jnp.bfloat16)


def run_product(left, right, table, pair):
    total_rows, seq_total = left.shape
    groups, factor, part, cols = right.shape
    pair_rows = pair.shape[0]
    rows = math.gcd(pair_rows, 8)
    width = pair.shape[2]
    return pl.pallas_call(
        functools.partial(product_kernel, rows, seq_total),
        grid=(pair_rows // rows,),
        in_specs=[
            pl.BlockSpec((rows * factor, seq_total), lambda b: (b, 0)),
            pl.BlockSpec(right.shape, lambda b: (0, 0, 0, 0), pipeline_mode=pl.Buffered(1)),
            pl.BlockSpec(table.shape, lambda b: (0, 0), pipeline_mode=pl.Buffered(1)),
            pl.BlockSpec((rows, cols, width), lambda b: (b, 0, 0)),
        ],
        out_specs=pl.BlockSpec((rows, cols, width), lambda b: (b, 0, 0)),
        out_shape=jax.ShapeDtypeStruct(pair.shape, jnp.bfloat16),
        scratch_shapes=[pltpu.VMEM((rows, factor * factor, cols), jnp.bfloat16)],
        compiler_params=pltpu.CompilerParams(
            dimension_semantics=("arbitrary",), vmem_limit_bytes=VMEM_LIMIT
        ),
        cost_estimate=pl.CostEstimate(
            flops=4 * total_rows * cols * factor * (seq_total + width),
            bytes_accessed=2 * (right.size + left.size + 2 * pair.size),
            transcendentals=0,
        ),
        name="product",
    )(left, right, table, pair)


def on_device(
    aligned_activity,
    pair_state,
    focus_scaling_vector,
    combined_probe_matrix,
    sigmoid_offset_vector,
    focus_final_matrix,
    pair_norm_gain,
    pair_bias_matrix,
    feedforward_scaling_vector,
    feedforward_widen_matrix,
    feedforward_shrink_matrix,
    tensor_scaling_vector,
    twin_operand_matrix,
    tensor_final_matrix,
):
    width = aligned_activity.shape[2]
    heads = pair_bias_matrix.shape[1]
    factor = twin_operand_matrix.shape[1] // 2
    res_axis = lax.axis_size("res")
    seq_axis = lax.axis_size("seq")
    rows = aligned_activity.shape[1]
    seq_count = aligned_activity.shape[0] // res_axis
    length = rows * res_axis
    col_block = pair_state.shape[1]
    chunks = math.gcd(CHUNKS, seq_count)
    per_chunk = seq_count // chunks
    pack = math.gcd(per_chunk, 128 // factor)

    pieces = aligned_activity.reshape(res_axis, seq_count, rows, width)
    arrived = [
        lax.all_to_all(
            pieces[:, c * per_chunk : (c + 1) * per_chunk], "res", split_axis=0, concat_axis=0, tiled=True
        )
        for c in range(chunks)
    ]

    pair_norm = layer_normalize(pair_state.astype(jnp.float32), pair_norm_gain)
    bias_tile = jnp.einsum(
        "ijc,ch->hij", pair_norm, pair_bias_matrix, precision=lax.Precision.HIGHEST
    ).astype(jnp.bfloat16)
    bias_cols = lax.all_gather(bias_tile, "seq", axis=2, tiled=True)
    bias_all = lax.all_gather(bias_cols, "res", axis=1, tiled=True)
    bias = bias_all.transpose(0, 2, 1).astype(jnp.float32) * LOG2E

    left_w = twin_operand_matrix[:, :factor]
    left_w = jnp.stack(
        [jnp.pad(left_w, ((0, 0), (t * factor, (pack - 1 - t) * factor))) for t in range(pack)]
    )
    weights = (
        focus_scaling_vector.reshape(1, -1),
        combined_probe_matrix.T,
        sigmoid_offset_vector.reshape(-1, 1),
        focus_final_matrix,
        feedforward_scaling_vector.reshape(1, -1),
        feedforward_widen_matrix,
        feedforward_shrink_matrix,
        tensor_scaling_vector.reshape(1, -1),
        left_w,
        twin_operand_matrix[:, factor:].T,
    )
    returned, lefts, rights = [], [], []
    for c in range(chunks):
        updated, left, right = run_sequences(arrived[c], bias, weights, heads, pack)
        returned.append(
            lax.all_to_all(updated, "res", split_axis=0, concat_axis=0, tiled=True)
        )
        lefts.append(left)
        rights.append(right)
    alignment_output = jnp.concatenate(returned, axis=1).reshape(aligned_activity.shape)

    left = lax.all_to_all(
        jnp.concatenate(lefts, axis=1), "res", split_axis=0, concat_axis=0, tiled=True
    )
    left = lax.all_gather(left, "seq", axis=0)
    left = left.reshape(seq_axis, res_axis, seq_count // pack, rows, pack, factor)
    left = left.transpose(3, 5, 1, 0, 2, 4).reshape(rows * factor, -1)

    right = jnp.concatenate(rights, axis=1).reshape(factor, seq_count, seq_axis, col_block)
    right = right.transpose(2, 0, 1, 3)
    right = lax.all_to_all(right, "seq", split_axis=0, concat_axis=0, tiled=True)
    right = lax.all_gather(right, "res", axis=0, tiled=True)
    if seq_count % 16 != 0:
        right = right.transpose(1, 0, 2, 3).reshape(1, factor, -1, col_block)
        right = right.reshape(1, factor, -1, col_block)
    table = tensor_final_matrix.reshape(factor, factor, -1).transpose(2, 1, 0)
    table = table.reshape(table.shape[0], -1)
    pair_output = run_product(left, right, table, pair_state)
    return (alignment_output, pair_output)


def solution(mesh):
    return jax.shard_map(
        on_device,
        mesh=mesh,
        in_specs=(
            P(("grp", "seq"), "res", None),
            P(("grp", "res"), "seq", None),
            P(),
            P(),
            P(),
            P(),
            P(),
            P(),
            P(),
            P(),
            P(),
            P(),
            P(),
            P(),
        ),
        out_specs=(P(("grp", "seq"), "res", None), P(("grp", "res"), "seq", None)),
        check_vma=False,
    )
```

```python
import functools
import math

import jax
import jax.numpy as jnp
from jax import lax
from jax.experimental import pallas as pl
from jax.experimental.pallas import tpu as pltpu
from jax.sharding import PartitionSpec as P

LOG2E = math.log2(math.e)
VMEM_LIMIT = 60 * 1024 * 1024
CHUNKS = 4
GROUPS = 2


def layer_normalize(inputs, scale_gain):
    sample_expectation = jnp.mean(inputs, axis=-1, keepdims=True)
    centered = inputs - sample_expectation
    variance = jnp.mean(centered * centered, axis=-1, keepdims=True)
    return centered * lax.rsqrt(variance + 1e-05) * scale_gain


def dot_f32(a, b, ca, cb):
    return lax.dot_general(a, b, (((ca,), (cb,)), ((), ())), preferred_element_type=jnp.float32)


def sequence_kernel(
    heads,
    pack,
    blocks,
    *refs,
):
    rank_ref, refs = refs[0], refs[1:]
    x_refs, refs = refs[:blocks], refs[blocks:]
    weight_refs, refs = refs[:11], refs[11:]
    out_refs, (right_ref, gathered, left_acc, right_acc) = refs[:blocks], refs[blocks:]
    (
        bias_ref,
        gain_ref,
        probe_ref,
        offset_ref,
        final_ref,
        ff_gain_ref,
        widen_ref,
        shrink_ref,
        opm_gain_ref,
        left_w_ref,
        right_w_ref,
    ) = weight_refs
    rank = rank_ref[0]
    step = pl.program_id(0)
    steps = right_ref.shape[2]
    _, rows, width = x_refs[0].shape
    length = blocks * rows
    depth = width // heads
    for d in range(blocks):
        gathered[lax.rem(rank + blocks - d, blocks)] = x_refs[d][0]
    x = gathered[...].astype(jnp.float32).reshape(length, width)
    normed = layer_normalize(x, gain_ref[...]).astype(jnp.bfloat16)
    mapped = dot_f32(probe_ref[...], normed, 1, 1)
    q = (mapped[:width] * (depth ** (-0.5) * LOG2E)).astype(jnp.bfloat16)
    k = mapped[width : 2 * width].astype(jnp.bfloat16)
    v = mapped[2 * width : 3 * width].astype(jnp.bfloat16)
    gate = jax.nn.sigmoid(mapped[3 * width :] + offset_ref[...])
    ones = jnp.ones((16, length), jnp.bfloat16)
    gated = []
    for h in range(heads):
        part = slice(h * depth, (h + 1) * depth)
        scores = dot_f32(k[part], q[part], 0, 0) + bias_ref[h]
        top = jnp.max(scores, axis=0, keepdims=True)
        p = jnp.exp2(scores - top).astype(jnp.bfloat16)
        mixed = dot_f32(jnp.concatenate([v[part], ones], axis=0), p, 1, 0)
        share = mixed[:depth] / mixed[depth : depth + 1]
        gated.append((share * gate[part]).astype(jnp.bfloat16))
    gated = jnp.concatenate(gated, axis=0)
    stream = x + dot_f32(gated, final_ref[...], 0, 0)
    normed = layer_normalize(stream, ff_gain_ref[...]).astype(jnp.bfloat16)
    hidden = jnp.maximum(dot_f32(normed, widen_ref[...], 1, 0), 0.0).astype(jnp.bfloat16)
    stream = stream + dot_f32(hidden, shrink_ref[...], 1, 0)
    updated = stream.astype(jnp.bfloat16)
    gathered[...] = stream.reshape(blocks, rows, width).astype(jnp.bfloat16)
    for d in range(blocks):
        out_refs[d][step] = gathered[lax.rem(rank + d, blocks)]
    normed = layer_normalize(updated.astype(jnp.float32), opm_gain_ref[...]).astype(jnp.bfloat16)
    slot = lax.rem(step, pack)
    left = dot_f32(normed, left_w_ref[slot], 1, 0).reshape(left_acc.shape)

    @pl.when(slot == 0)
    def _():
        left_acc[...] = left

    @pl.when(slot != 0)
    def _():
        left_acc[...] = left_acc[...] + left

    factor = right_w_ref.shape[0]
    right = dot_f32(right_w_ref[...], normed, 1, 1)
    for e in range(factor):
        right_acc[e, pl.ds(step, 1), :] = right[e : e + 1]

    @pl.when(step == steps - 1)
    def _():
        lanes = left_acc.shape[2]
        cols = right_ref.shape[3]
        for part in range(right_ref.shape[0]):
            right_ref[part] = right_acc[:, :, part * cols : (part + 1) * cols].astype(jnp.bfloat16)
        for d in range(blocks):
            if lanes < width:
                out_refs[d][steps] = jnp.zeros((rows, width), jnp.bfloat16)
            out_refs[d][steps, :, :lanes] = left_acc[lax.rem(rank + d, blocks)].astype(jnp.bfloat16)


def run_sequences(rank, xs, bias, weights, heads, pack, halves):
    blocks = len(xs)
    steps, rows, width = xs[0].shape
    length = blocks * rows
    factor = weights[-1].shape[0]
    cols = length // halves
    whole = lambda a: pl.BlockSpec(
        a.shape, lambda s, n=a.ndim: (0,) * n, pipeline_mode=pl.Buffered(1)
    )
    kept = lambda shape: pl.BlockSpec(shape, lambda s, n=len(shape): (0,) * n)
    lanes = pack * factor
    hidden = weights[5].shape[1]
    flops = 2 * length * width * (5 * width + 2 * hidden + 128) + 4 * length * length * width
    shapes = [(steps + 1, rows, width)] * blocks + [(halves, factor, steps, cols)]
    return pl.pallas_call(
        functools.partial(sequence_kernel, heads, pack, blocks),
        grid=(steps,),
        in_specs=[pl.BlockSpec(memory_space=pltpu.SMEM)]
        + [pl.BlockSpec((1, rows, width), lambda s: (s, 0, 0)) for _ in xs]
        + [whole(a) for a in (bias,) + weights],
        out_specs=[kept(a) for a in shapes],
        out_shape=[jax.ShapeDtypeStruct(a, jnp.bfloat16) for a in shapes],
        scratch_shapes=[
            pltpu.VMEM((blocks, rows, width), jnp.bfloat16),
            pltpu.VMEM((blocks, rows, lanes), jnp.float32),
            pltpu.VMEM((factor, steps, length), jnp.float32),
        ],
        compiler_params=pltpu.CompilerParams(
            dimension_semantics=("arbitrary",), vmem_limit_bytes=VMEM_LIMIT
        ),
        cost_estimate=pl.CostEstimate(
            flops=steps * flops * 3,
            bytes_accessed=bias.size * 4 + 4 * length * width * steps,
            transcendentals=steps * heads * length * length,
        ),
        name="sequences",
    )(rank, *xs, bias, *weights)


def deal_kernel(chunks, rank_ref, x_ref, *out_refs):
    blocks = x_ref.shape[0]
    part = x_ref.shape[1] // chunks
    for c in range(chunks):
        for d in range(blocks):
            source = lax.rem(rank_ref[0] + d, blocks)
            out_refs[c * blocks + d][...] = x_ref[source, c * part : (c + 1) * part]


def collect_kernel(chunks, rank_ref, *refs):
    in_refs, (out_ref, left_ref) = refs[:-2], refs[-2:]
    blocks = out_ref.shape[0]
    part = out_ref.shape[1] // chunks
    lanes = left_ref.shape[3]
    for c in range(chunks):
        for d in range(blocks):
            target = lax.rem(rank_ref[0] + blocks - d, blocks)
            y_ref = in_refs[c * blocks + d]
            out_ref[target, c * part : (c + 1) * part] = y_ref[:part]
            left_ref[target, c] = y_ref[part, :, :lanes]


def vmem_call(kernel, shapes, rank, arrays, name):
    return pl.pallas_call(
        kernel,
        in_specs=[pl.BlockSpec(memory_space=pltpu.SMEM)]
        + [pl.BlockSpec(memory_space=pltpu.VMEM)] * len(arrays),
        out_specs=[pl.BlockSpec(memory_space=pltpu.VMEM)] * len(shapes),
        out_shape=[jax.ShapeDtypeStruct(a, jnp.bfloat16) for a in shapes],
        compiler_params=pltpu.CompilerParams(vmem_limit_bytes=VMEM_LIMIT // 2),
        cost_estimate=pl.CostEstimate(
            flops=0, bytes_accessed=4 * sum(a.size for a in arrays), transcendentals=0
        ),
        name=name,
    )(rank, *arrays)


def shift_all(arrays):
    size = len(arrays)
    return [arrays[0]] + [
        lax.ppermute(arrays[d], "res", [(r, (r + d) % size) for r in range(size)])
        for d in range(1, size)
    ]


def product_kernel(rows, seq_total, left_ref, *refs):
    right_refs, (table_ref, pair_ref, out_ref, stack) = refs[:-4], refs[-4:]
    groups, factor, part, cols = right_refs[0].shape
    scale = 1.0 / seq_total
    left = left_ref[...]
    for e in range(factor):
        right = jnp.concatenate(
            [ref[:, e].reshape(groups * part, cols) for ref in right_refs], axis=0
        )
        outer = (dot_f32(left, right, 1, 0) * scale).astype(jnp.bfloat16)
        stack[:, e * factor : (e + 1) * factor, :] = outer.reshape(rows, factor, cols)
    for i in range(rows):
        update = dot_f32(table_ref[...], stack[i], 1, 0)
        out_ref[i] = (pair_ref[i].astype(jnp.float32) + update.T).astype(jnp.bfloat16)


def run_product(left, rights, table, pair):
    total_rows, seq_total = left.shape
    _, factor, _, cols = rights[0].shape
    pair_rows = pair.shape[0]
    rows = math.gcd(pair_rows, 8)
    width = pair.shape[2]
    return pl.pallas_call(
        functools.partial(product_kernel, rows, seq_total),
        grid=(pair_rows // rows,),
        in_specs=[
            pl.BlockSpec((rows * factor, seq_total), lambda b: (b, 0)),
            *[
                pl.BlockSpec(a.shape, lambda b: (0, 0, 0, 0), pipeline_mode=pl.Buffered(1))
                for a in rights
            ],
            pl.BlockSpec(table.shape, lambda b: (0, 0), pipeline_mode=pl.Buffered(1)),
            pl.BlockSpec((rows, cols, width), lambda b: (b, 0, 0)),
        ],
        out_specs=pl.BlockSpec((rows, cols, width), lambda b: (b, 0, 0)),
        out_shape=jax.ShapeDtypeStruct(pair.shape, jnp.bfloat16),
        scratch_shapes=[pltpu.VMEM((rows, factor * factor, cols), jnp.bfloat16)],
        compiler_params=pltpu.CompilerParams(
            dimension_semantics=("arbitrary",), vmem_limit_bytes=VMEM_LIMIT
        ),
        cost_estimate=pl.CostEstimate(
            flops=4 * total_rows * cols * factor * (seq_total + width),
            bytes_accessed=2 * (left.size * (1 + cols * factor // total_rows) + left.size + 2 * pair.size),
            transcendentals=0,
        ),
        name="product",
    )(left, *rights, table, pair)


def on_device(
    aligned_activity,
    pair_state,
    focus_scaling_vector,
    combined_probe_matrix,
    sigmoid_offset_vector,
    focus_final_matrix,
    pair_norm_gain,
    pair_bias_matrix,
    feedforward_scaling_vector,
    feedforward_widen_matrix,
    feedforward_shrink_matrix,
    tensor_scaling_vector,
    twin_operand_matrix,
    tensor_final_matrix,
):
    width = aligned_activity.shape[2]
    heads = pair_bias_matrix.shape[1]
    factor = twin_operand_matrix.shape[1] // 2
    res_axis = lax.axis_size("res")
    seq_axis = lax.axis_size("seq")
    rows = aligned_activity.shape[1]
    seq_count = aligned_activity.shape[0] // res_axis
    length = rows * res_axis
    col_block = pair_state.shape[1]
    chunks = math.gcd(CHUNKS, seq_count)
    per_chunk = seq_count // chunks
    pack = per_chunk

    groups = math.gcd(GROUPS, chunks) if seq_count % (8 * GROUPS) == 0 else 1
    rank = lax.axis_index("res").astype(jnp.int32).reshape(1)
    pieces = aligned_activity.reshape(res_axis, seq_count, rows, width)
    dealt = vmem_call(
        functools.partial(deal_kernel, chunks),
        [(per_chunk, rows, width)] * (chunks * res_axis),
        rank,
        [pieces],
        "deal",
    )
    arrived = [shift_all(dealt[c * res_axis : (c + 1) * res_axis]) for c in range(chunks)]

    pair_norm = layer_normalize(pair_state.astype(jnp.float32), pair_norm_gain)
    bias_tile = jnp.einsum(
        "ijc,ch->hij", pair_norm, pair_bias_matrix, precision=lax.Precision.HIGHEST
    ).astype(jnp.bfloat16)
    bias_rows = lax.all_gather(bias_tile, "res", axis=1, tiled=True)
    bias_all = lax.all_gather(bias_rows, "seq", axis=0)
    bias = bias_all.transpose(1, 0, 3, 2).reshape(heads, length, length)
    bias = bias.astype(jnp.float32) * LOG2E

    left_w = twin_operand_matrix[:, :factor]
    left_w = jnp.stack(
        [jnp.pad(left_w, ((0, 0), (t * factor, (pack - 1 - t) * factor))) for t in range(pack)]
    )
    weights = (
        focus_scaling_vector.reshape(1, -1),
        combined_probe_matrix.T,
        sigmoid_offset_vector.reshape(-1, 1),
        focus_final_matrix,
        feedforward_scaling_vector.reshape(1, -1),
        feedforward_widen_matrix,
        feedforward_shrink_matrix,
        tensor_scaling_vector.reshape(1, -1),
        left_w,
        twin_operand_matrix[:, factor:].T,
    )
    returned, rights, pending = [], [], []
    for c in range(chunks):
        *updated, right = run_sequences(rank, arrived[c], bias, weights, heads, pack, seq_axis)
        returned += shift_all(updated)
        pending.append(right)
        if len(pending) == chunks // groups:
            right = jnp.concatenate(pending, axis=2)
            right = lax.all_to_all(right, "seq", split_axis=0, concat_axis=0, tiled=True)
            rights.append(lax.all_gather(right, "res", axis=0, tiled=True))
            pending = []
    if (seq_count // groups) % 8 != 0:
        rights = [r.transpose(1, 0, 2, 3).reshape(1, factor, -1, col_block) for r in rights]
    alignment_output, left = vmem_call(
        functools.partial(collect_kernel, chunks),
        [pieces.shape, (res_axis, chunks, rows, pack * factor)],
        rank,
        returned,
        "collect",
    )
    alignment_output = alignment_output.reshape(aligned_activity.shape)
    left = lax.all_gather(left, "seq", axis=0)
    left = left.reshape(seq_axis, res_axis, groups, chunks // groups, rows, pack, factor)
    left = left.transpose(4, 6, 2, 1, 0, 3, 5).reshape(rows * factor, -1)

    table = tensor_final_matrix.reshape(factor, factor, -1).transpose(2, 1, 0)
    table = table.reshape(table.shape[0], -1)
    pair_output = run_product(left, rights, table, pair_state)
    return (alignment_output, pair_output)


def solution(mesh):
    return jax.shard_map(
        on_device,
        mesh=mesh,
        in_specs=(
            P(("grp", "seq"), "res", None),
            P(("grp", "res"), "seq", None),
            P(),
            P(),
            P(),
            P(),
            P(),
            P(),
            P(),
            P(),
            P(),
            P(),
            P(),
            P(),
        ),
        out_specs=(P(("grp", "seq"), "res", None), P(("grp", "res"), "seq", None)),
        check_vma=False,
    )
```
